32 devices in a mesh: gx: 2 (over x), gy: 4 (over z), gz: 4 (over y, core).
Axes of the slice: x: 2, y: 2, z: 4, core: 2. Of those that a mesh axis runs over, the one named last changes fastest.
Arguments:
- partials: float32 [32, 32, 64, 512], P('gx', None, 'gy', 'gz'), may hold values from -40 to 40
- code_bits: int32 [32, 32], replicated, may hold values from 0 to 1
- group_map: int32 [32], replicated, may hold values from 0 to 31, each once
- velocity: float32 [32, 64, 512], P('gx', 'gy', 'gz'), may hold values from 1.5 to 4.5
Outputs:
- gradient: float32 [32, 64, 512], P('gx', 'gy', 'gz')
- new_model: float32 [32, 64, 512], P('gx', 'gy', 'gz')
The draws below stay inside these ranges and needn't reach their ends.
Inputs may be any that keep to these rules, and one draw needn't show every extreme that they name: `group_map`: every group of 0 to 31 stands in exactly one slot.
All inputs are finite; a program needn't handle non-finite values.
Results may differ from the reference program's by a relative error of at most 0.0001.
Values sent between devices are 32-bit elements; how exact they have to be, the bound alone decides.
A program may use at most 64 MiB of HBM per device.

```python
import jax
import jax.numpy as jnp
from jax import lax

G = 32
ITERS = 3
NX = 32
NY = 64
NZ = 512


def draw_partials(key, part):
    first_key = jax.random.fold_in(jax.random.fold_in(key, 17), 0)
    rough = jnp.clip(jax.random.normal(first_key, (G, NX, NY, NZ), jnp.float32), -6.0, 6.0)
    return rough


def set_ends(result, rng, smallest, top_value):
    longest = result.shape.index(max(result.shape))
    spots = []
    for shift in (0, 1):
        where = [jax.random.randint(jax.random.fold_in(rng, axis), (), 0, length) for axis, length in enumerate(result.shape)]
        where[longest] = (where[longest] + shift) % result.shape[longest]
        spots.append(tuple(where))
    return result.at[spots[0]].set(smallest).at[spots[1]].set(top_value)


def block_scale(key, dims, pieces, low, top_value):
    def one(axis_at, parts):
        draws = jax.random.uniform(jax.random.fold_in(jax.random.fold_in(key, 6), axis_at), (parts,), jnp.float32, low / len(pieces), top_value / len(pieces))
        return jnp.repeat(jnp.exp(draws), dims[axis_at] // parts).reshape((-1,) + (1,) * (len(dims) - axis_at - 1))

    loudness = one(*pieces[0])
    for cut in pieces[1:]:
        loudness = loudness * one(*cut)
    return loudness


def setup_inputs(seed: int = 0) -> dict:
    arg_keys = jax.random.split(jax.random.key(seed), 5)
    return {
        "partials": draw_partials(jax.random.fold_in(arg_keys[4], 71), 0),
        "code_bits": set_ends(jax.random.randint(arg_keys[1], (G, NX), 0, 2), jax.random.fold_in(arg_keys[1], 1), 0, 1).astype(jnp.int32),
        "group_map": jax.random.permutation(arg_keys[2], G).astype(jnp.int32),
        "velocity": jnp.clip(1.5 + 3.0 * jax.random.uniform(arg_keys[3], (NX, NY, NZ), jnp.float32) ** block_scale(arg_keys[3], (NX, NY, NZ), ((0, 2), (1, 4), (2, 4)), -0.2, 0.2), 1.5, 4.5),
    }


step_length = 0.5
tv_weight = 0.2
dual_step = 0.28
primal_step = 0.28

def forward_diff(field):
    zeros_x = jnp.zeros((1,) + field.shape[1:], jnp.float32)
    zeros_y = jnp.zeros((field.shape[0], 1, field.shape[2]), jnp.float32)
    zeros_z = jnp.zeros(field.shape[:2] + (1,), jnp.float32)
    diff_x = jnp.concatenate([field[1:] - field[:-1], zeros_x], 0)
    diff_y = jnp.concatenate([field[:, 1:] - field[:, :-1], zeros_y], 1)
    diff_z = jnp.concatenate([field[:, :, 1:] - field[:, :, :-1], zeros_z], 2)
    return jnp.stack([diff_x, diff_y, diff_z])

def divergence(dual_field):
    left_x = jnp.pad(dual_field[0][:-1], ((1, 0), (0, 0), (0, 0)))
    left_y = jnp.pad(dual_field[1][:, :-1], ((0, 0), (1, 0), (0, 0)))
    left_z = jnp.pad(dual_field[2][:, :, :-1], ((0, 0), (0, 0), (1, 0)))
    return dual_field[0] - left_x + (dual_field[1] - left_y) + (dual_field[2] - left_z)

def reference(partials, code_bits, group_map, velocity):
    sign_table = 2.0 * code_bits[group_map].astype(jnp.float32) - 1.0

    def accumulate(index, acc):
        return acc + sign_table[index][:, None, None] * partials[index]
    gradient = lax.fori_loop(0, partials.shape[0], accumulate, jnp.zeros(velocity.shape, jnp.float32))
    mean_square = jnp.sum(gradient * gradient) / gradient.size
    step_scale = step_length / jnp.sqrt(mean_square + 1.0)
    target = velocity - step_scale * gradient
    current = target
    extra = target
    dual_field = jnp.zeros((3,) + target.shape, jnp.float32)
    for iteration in range(ITERS):
        dual_field = dual_field + dual_step * forward_diff(extra)
        magnitude = jnp.sqrt(lax.optimization_barrier(jnp.sum(dual_field * dual_field, axis=0)))
        dual_field = dual_field / jnp.maximum(1.0, magnitude / tv_weight)[None]
        updated = (current + primal_step * divergence(dual_field) + primal_step * target) / (1.0 + primal_step)
        extra = 2.0 * updated - current
        current = updated
    return (gradient, current)
```

```python
import functools

import jax
import jax.numpy as jnp
from jax import lax
from jax.experimental import pallas as pl
from jax.experimental.pallas import tpu as pltpu
from jax.sharding import PartitionSpec as P

ITERS = 3
H = ITERS
SEG = 16
PIECES = 2

step_length = 0.5
tv_weight = 0.2
dual_step = 0.28
primal_step = 0.28
MESH = pl.DeviceIdType.MESH


def kernel(
    dims,
    partials,
    code_bits,
    group_map,
    velocity,
    gradient_out,
    model_out,
    bits,
    gmap,
    part,
    psum,
    vw,
    gw,
    xr,
    xh,
    ys,
    yr,
    ss,
    zr,
    ds,
    dr,
    za,
    va,
    ga,
    target,
    current,
    extra,
    dx,
    dy,
    dz,
    ar,
    result,
    in_sem,
    part_sem,
    xs_sem,
    xr_sem,
    xhs_sem,
    xhr_sem,
    vs_sem,
    vr_sem,
    hs_sem,
    hr_sem,
    ars_sem,
    arr_sem,
    out_sem,
    chain_sem,
):
    nx, ny, nz, slots, bx, by, bz = dims
    rows_all = nx * bx
    sides = min(2, nx - 1)
    win = bx + H * sides
    groups = bz // SEG
    tiles = -(-win // groups)
    yp = -(-(by + 2 * H) // 8) * 8
    ix, iy, iz = lax.axis_index("gx"), lax.axis_index("gy"), lax.axis_index("gz")

    def offset(q):
        return jnp.where(q == 0, 0, jnp.where(q == nx - 1, win - bx, H)) if nx > 1 else 0

    off = offset(ix)
    size = bx // PIECES
    order = [(d, p) for d in list(range(1, nx)) + [0] for p in range(PIECES)]

    def first_row(d, p):
        return lax.rem(ix + d, nx) * bx + p * size

    in_copies = [
        pltpu.make_async_copy(code_bits, bits, in_sem.at[0]),
        pltpu.make_async_copy(group_map, gmap, in_sem.at[1]),
    ]
    v_copy = pltpu.make_async_copy(velocity, vw.at[pl.ds(off, bx)], in_sem.at[2])
    for c in in_copies:
        c.start()
    part_copies = []
    for n, (d, p) in enumerate(order):
        where = pl.ds(first_row(d, p), size)
        part_copies.append(
            pltpu.make_async_copy(partials.at[:, where], part.at[:, where], part_sem.at[n])
        )
    for c in part_copies:
        c.start()
    v_copy.start()

    barrier = pltpu.get_barrier_semaphore()

    def at(x=None, y=None, z=None):
        return (ix if x is None else x, iy if y is None else y, iz if z is None else z)

    def notify(sem, device):
        pl.semaphore_signal(sem, inc=1, device_id=device, device_id_type=MESH)

    for buffer in (yr, zr, dr, va, ga, za, xh, dx, dy, dz, extra, target, current):
        buffer[...] = jnp.zeros_like(buffer)

    if nx > 1:
        @pl.when(ix > 0)
        def _():
            for r in range(H):
                vw[off - H + r] = jnp.zeros((by, bz), jnp.float32)

        @pl.when(ix < nx - 1)
        def _():
            for r in range(H):
                vw[off + bx + r] = jnp.zeros((by, bz), jnp.float32)

    for d in range(1, nx):
        notify(barrier, at(x=lax.rem(ix + d, nx)))
    has = {
        "y-": iy > 0,
        "y+": iy < ny - 1,
        "z-": iz > 0,
        "z+": iz < nz - 1,
    }
    near = {
        "y-": at(y=iy - 1),
        "y+": at(y=iy + 1),
        "z-": at(z=iz - 1),
        "z+": at(z=iz + 1),
    }
    total = jnp.int32(nx - 1)
    for key in has:
        total = total + has[key].astype(jnp.int32)

        @pl.when(has[key])
        def _(key=key):
            notify(barrier, near[key])

    for c in in_copies:
        c.wait()
    pl.semaphore_wait(barrier, total)

    codes = [gmap[ix * slots + s] for s in range(slots)]

    def reduce_rows(first):
        def one(r, carry):
            row = first + r
            acc = None
            for s in range(slots):
                sign = (2 * bits[codes[s], row] - 1).astype(jnp.float32)
                term = sign * part[s, row]
                acc = term if acc is None else acc + term
            psum[row] = acc
            return carry

        lax.fori_loop(0, size, one, 0, unroll=2)

    def x_copy(d, p):
        return pltpu.make_async_remote_copy(
            src_ref=psum.at[pl.ds(first_row(d, p), size)],
            dst_ref=xr.at[d - 1, pl.ds(p * size, size)],
            send_sem=xs_sem.at[d - 1, p],
            recv_sem=xr_sem.at[d - 1, p],
            device_id=at(x=lax.rem(ix + d, nx)),
            device_id_type=MESH,
        )

    for n, (d, p) in enumerate(order):
        part_copies[n].wait()
        reduce_rows(first_row(d, p))
        if d > 0:
            x_copy(d, p).start()

    def halo_copy(d, side):
        q = lax.rem(ix + d, nx)
        first = q * bx - H if side == 0 else q * bx + bx
        return pltpu.make_async_remote_copy(
            src_ref=psum.at[pl.ds(first, H)],
            dst_ref=xh.at[d - 1, side],
            send_sem=xhs_sem.at[d - 1, side],
            recv_sem=xhr_sem.at[d - 1, side],
            device_id=at(x=q),
            device_id_type=MESH,
        )

    def v_halo(side):
        q = ix + 1 if side == 0 else ix - 1
        src = off + bx - H if side == 0 else off
        dst = offset(q) - H if side == 0 else offset(q) + bx
        return pltpu.make_async_remote_copy(
            src_ref=vw.at[pl.ds(src, H)],
            dst_ref=vw.at[pl.ds(dst, H)],
            send_sem=vs_sem.at[side],
            recv_sem=vr_sem.at[side],
            device_id=at(x=q),
            device_id_type=MESH,
        )

    v_copy.wait()
    for d in range(1, nx):
        q = lax.rem(ix + d, nx)

        @pl.when(q > 0)
        def _(d=d):
            halo_copy(d, 0).start()

        @pl.when(q < nx - 1)
        def _(d=d):
            halo_copy(d, 1).start()

    if nx > 1:
        @pl.when(ix < nx - 1)
        def _():
            v_halo(0).start()

        @pl.when(ix > 0)
        def _():
            v_halo(1).start()

    def chain(up, down, count, index, sems):
        if count == 1:
            return

        @pl.when(index > 0)
        def _():
            pl.semaphore_wait(chain_sem.at[sems], 1)

        @pl.when(index < count - 1)
        def _():
            notify(chain_sem.at[sems], up)
            pl.semaphore_wait(chain_sem.at[sems + 1], 1)

        @pl.when(index > 0)
        def _():
            notify(chain_sem.at[sems + 1], down)

    chain(near["y+"], near["y-"], ny, iy, 0)
    chain(near["z+"], near["z-"], nz, iz, 2)
    for d in range(1, nx):
        notify(chain_sem.at[4], at(x=lax.rem(ix + d, nx)))

    squares = jnp.zeros((by, bz), jnp.float32)
    for p in range(PIECES):
        for d in range(1, nx):
            x_copy(d, p).wait_recv()
        for r in range(p * size, (p + 1) * size):
            row = psum[ix * bx + r]
            for d in range(1, nx):
                row = row + xr[d - 1, r]
            gw[off + r] = row
            squares = squares + row * row
    count = nx * ny * nz
    me = (ix * ny + iy) * nz + iz
    ar[me] = jnp.sum(squares, axis=0, keepdims=True)
    if nx > 1:
        pl.semaphore_wait(chain_sem.at[4], nx - 1)

    def send_square(d, carry):
        other = lax.rem(me + d, count)
        pltpu.make_async_remote_copy(
            src_ref=ar.at[me],
            dst_ref=ar.at[me],
            send_sem=ars_sem,
            recv_sem=arr_sem,
            device_id=(other // (ny * nz), lax.rem(other // nz, ny), lax.rem(other, nz)),
            device_id_type=MESH,
        ).start()
        return carry

    lax.fori_loop(1, count, send_square, 0)
    g_out = pltpu.make_async_copy(gw.at[pl.ds(off, bx)], gradient_out, out_sem.at[0])
    g_out.start()

    for side in range(2):
        if nx == 1:
            break
        present = ix > 0 if side == 0 else ix < nx - 1

        @pl.when(present)
        def _(side=side):
            for d in range(1, nx):
                zone = xh.at[d - 1, side]
                pltpu.make_async_copy(zone, zone, xhr_sem.at[d - 1, side]).wait()
            zone = vw.at[pl.ds(off - H if side == 0 else off + bx, H)]
            pltpu.make_async_copy(zone, zone, vr_sem.at[side]).wait()
            for r in range(H):
                there = ix * bx - H + r if side == 0 else ix * bx + bx + r
                row = psum[there]
                for d in range(1, nx):
                    row = row + xh[d - 1, side, r]
                gw[(off - H if side == 0 else off + bx) + r] = row

    lane = lax.broadcasted_iota(jnp.int32, (1, bz), 1)
    group = lane // SEG
    spot = lax.rem(lane, SEG)

    def roll(value, shift):
        shift = shift % bz
        return value if shift == 0 else pltpu.roll(value, shift, 1)

    def pack(read, k):
        acc = None
        for g in range(groups):
            x = tiles * g + k
            if x >= win:
                continue
            moved = roll(read(x), H + SEG * g)
            acc = moved if acc is None else jnp.where(group == g, moved, acc)
        return acc

    fields = (vw, gw)
    for f, field in enumerate(fields):
        for x in range(win):
            tile = field[x]
            ys[0, f, x * H : x * H + H] = tile[by - H : by]
            ys[1, f, x * H : x * H + H] = tile[0:H]
        for k in range(tiles):
            tile = pack(lambda x: field[x], k)
            ss[f, k] = tile
            ds[0, f, k * H : k * H + H] = tile[by - H : by]
            ds[1, f, k * H : k * H + H] = tile[0:H]

    def send(src, dst, n, device):
        return pltpu.make_async_remote_copy(
            src_ref=src,
            dst_ref=dst,
            send_sem=hs_sem.at[n],
            recv_sem=hr_sem.at[n],
            device_id=device,
            device_id_type=MESH,
        )

    both = lambda a, b: jnp.logical_and(has[a], has[b])
    exchange = [
        (send(ys.at[0], yr.at[0], 0, near["y+"]), has["y+"], has["y-"]),
        (send(ys.at[1], yr.at[1], 1, near["y-"]), has["y-"], has["y+"]),
        (send(ss, zr.at[0], 2, near["z+"]), has["z+"], has["z-"]),
        (send(ss, zr.at[1], 3, near["z-"]), has["z-"], has["z+"]),
        (send(ds.at[0], dr.at[0], 4, at(y=iy + 1, z=iz + 1)), both("y+", "z+"), both("y-", "z-")),
        (send(ds.at[0], dr.at[1], 5, at(y=iy + 1, z=iz - 1)), both("y+", "z-"), both("y-", "z+")),
        (send(ds.at[1], dr.at[2], 6, at(y=iy - 1, z=iz + 1)), both("y-", "z+"), both("y+", "z-")),
        (send(ds.at[1], dr.at[3], 7, at(y=iy - 1, z=iz - 1)), both("y-", "z-"), both("y+", "z+")),
    ]
    for copy, sends, _ in exchange:
        pl.when(sends)(copy.start)
    for copy, _, receives in exchange:
        pl.when(receives)(copy.wait_recv)

    front = 8

    def base(x):
        return front + x * yp

    for f, (field, whole) in enumerate(((vw, va), (gw, ga))):
        for x in range(win):
            b = base(x)
            whole[b + H : b + H + by] = field[x]
            whole[b : b + H] = yr[0, f, x * H : x * H + H]
            whole[b + H + by : b + 2 * H + by] = yr[1, f, x * H : x * H + H]
        for k in range(tiles):
            for z in range(2):
                za[z, H : H + by] = zr[z, f, k]
                za[z, 0:H] = dr[z, f, k * H : k * H + H]
                za[z, H + by : 2 * H + by] = dr[2 + z, f, k * H : k * H + H]
            left = za[0, 0:yp]
            mine = pack(lambda x: whole[base(x) : base(x) + yp], k)
            right = roll(za[1, 0:yp], SEG // 2)
            b = base(win + k)
            whole[b : b + yp] = jnp.where(
                spot < H,
                left,
                jnp.where(
                    spot < SEG // 2,
                    mine,
                    jnp.where(spot < SEG // 2 + H, roll(mine, SEG // 2), right),
                ),
            )

    many = ar.at[pl.ds(0, count - 1)]
    pltpu.make_async_copy(many, many, arr_sem).wait()
    square_sum = jnp.sum(jnp.sum(ar[...], axis=0), axis=1, keepdims=True)
    cells = nx * ny * nz * bx * by * bz
    scale = step_length * lax.rsqrt(square_sum / cells + 1.0)

    y_at = iy * by - H + lax.broadcasted_iota(jnp.int32, (yp, 1), 0)
    keep_y = jnp.logical_and(y_at >= 0, y_at < ny * by - 1)
    keep_y = jnp.broadcast_to(keep_y, (yp, bz))
    z_main = iz * bz + lane
    keep_z_main = jnp.broadcast_to(z_main < nz * bz - 1, (yp, bz))
    z_pack = iz * bz + jnp.where(spot < SEG // 2, spot - H, spot - SEG // 2 + bz - H)
    keep_z_pack = jnp.broadcast_to(
        jnp.logical_and(z_pack >= 0, z_pack < nz * bz - 1), (yp, bz)
    )
    start = ix * bx - off
    blocks = win + tiles

    def rows(ref, x, shift=0):
        return ref[base(x) + shift : base(x) + shift + yp]

    for x in range(blocks):
        value = rows(va, x) - scale * rows(ga, x)
        target[base(x) : base(x) + yp] = value

    for it in range(ITERS):
        now = target if it == 0 else extra
        held = target if it == 0 else current
        last = it == ITERS - 1
        for x in range(blocks):
            here = rows(now, x)
            b = base(x)
            ddy = jnp.where(keep_y, rows(now, x, 1) - here, 0.0)
            if x < win:
                g, k = x // tiles, x % tiles
                edge = roll(rows(now, win + k), bz - 1 - (SEG * g + SEG // 2 + H))
                after = jnp.where(lane == bz - 1, edge, roll(here, -1))
                ddz = jnp.where(keep_z_main, after - here, 0.0)
                if x == win - 1:
                    ddx = jnp.zeros_like(here)
                else:
                    ddx = rows(now, x + 1) - here
            else:
                k = x - win
                ddz = jnp.where(keep_z_pack, roll(here, -1) - here, 0.0)
                if k < tiles - 1:
                    after = rows(now, x + 1)
                else:
                    after = roll(rows(now, win), -SEG)
                ddx = jnp.where(tiles * group + k < win - 1, after - here, 0.0)
            px, py, pz = dual_step * ddx, dual_step * ddy, dual_step * ddz
            if it > 0:
                px, py, pz = rows(dx, x) + px, rows(dy, x) + py, rows(dz, x) + pz
            shrink = jnp.minimum(1.0, tv_weight * lax.rsqrt(px * px + py * py + pz * pz))
            dx[b : b + yp] = px * shrink
            dy[b : b + yp] = py * shrink
            dz[b : b + yp] = pz * shrink
        for x in range(win if last else blocks):
            b = base(x)
            qx, qy, qz = rows(dx, x), rows(dy, x), rows(dz, x)
            spread = qy - rows(dy, x, -1)
            if x < win:
                g, k = x // tiles, x % tiles
                edge = roll(rows(dz, win + k), -(SEG * g + H - 1))
                spread = spread + (qz - jnp.where(lane == 0, edge, roll(qz, 1)))
                spread = spread + (qx if x == 0 else qx - rows(dx, x - 1))
            else:
                k = x - win
                spread = spread + (qz - roll(qz, 1))
                before = rows(dx, x - 1) if k > 0 else roll(rows(dx, blocks - 1), SEG)
                spread = spread + (qx - before)
            old = rows(held, x)
            new = (old + primal_step * (spread + rows(target, x))) * (1.0 / (1.0 + primal_step))
            if last:
                result[x] = new[H : H + by]
            else:
                current[b : b + yp] = new
                extra[b : b + yp] = 2.0 * new - old

    m_out = pltpu.make_async_copy(result.at[pl.ds(off, bx)], model_out, out_sem.at[1])
    m_out.start()

    for d in range(1, nx):
        for p in range(PIECES):
            x_copy(d, p).wait_send()
        q = lax.rem(ix + d, nx)
        pl.when(q > 0)(halo_copy(d, 0).wait_send)
        pl.when(q < nx - 1)(halo_copy(d, 1).wait_send)
    if nx > 1:
        pl.when(ix < nx - 1)(v_halo(0).wait_send)
        pl.when(ix > 0)(v_halo(1).wait_send)
    for copy, sends, _ in exchange:
        pl.when(sends)(copy.wait_send)
    pltpu.make_async_copy(many, many, ars_sem).wait()
    g_out.wait()
    m_out.wait()


def shards(partials, code_bits, group_map, velocity):
    slots = partials.shape[0]
    bx, by, bz = velocity.shape
    nx, ny, nz = (lax.axis_size(a) for a in ("gx", "gy", "gz"))
    dims = (nx, ny, nz, slots, bx, by, bz)
    win = bx + H * min(2, nx - 1)
    tiles = -(-win // (bz // SEG))
    yp = -(-(by + 2 * H) // 8) * 8
    flat = 16 + (win + tiles) * yp
    strip = -(-(win * H + 5) // 8) * 8
    diag = -(-(tiles * H + 5) // 8) * 8
    f32 = functools.partial(pltpu.VMEM, dtype=jnp.float32)
    peers = max(nx - 1, 1)
    dma = pltpu.SemaphoreType.DMA
    anywhere = pl.BlockSpec(memory_space=pl.ANY)
    block = jax.ShapeDtypeStruct(velocity.shape, jnp.float32)
    return pl.pallas_call(
        functools.partial(kernel, dims),
        out_shape=(block, block),
        in_specs=[anywhere] * 4,
        out_specs=(anywhere, anywhere),
        scratch_shapes=[
            pltpu.SMEM(code_bits.shape, jnp.int32),
            pltpu.SMEM(group_map.shape, jnp.int32),
            f32(partials.shape),
            f32((nx * bx, by, bz)),
            f32((win, by, bz)),
            f32((win, by, bz)),
            f32((peers, bx, by, bz)),
            f32((peers, 2, H, by, bz)),
            f32((2, 2, strip, bz)),
            f32((2, 2, strip, bz)),
            f32((2, tiles, by, bz)),
            f32((2, 2, tiles, by, bz)),
            f32((2, 2, diag, bz)),
            f32((4, 2, diag, bz)),
            f32((2, yp + 8, bz)),
        ]
        + [f32((flat, bz))] * 8
        + [
            f32((nx * ny * nz, 1, bz)),
            f32((win, by, bz)),
            dma((3,)),
            dma((nx * PIECES,)),
            dma((peers, PIECES)),
            dma((peers, PIECES)),
            dma((peers, 2)),
            dma((peers, 2)),
            dma((2,)),
            dma((2,)),
            dma((8,)),
            dma((8,)),
            dma,
            dma,
            dma((2,)),
            pltpu.SemaphoreType.REGULAR((5,)),
        ],
        compiler_params=pltpu.CompilerParams(collective_id=0, has_side_effects=True),
    )(partials, code_bits, group_map, velocity)


def solution(mesh):
    placed = (P("gx", None, "gy", "gz"), P(), P(), P("gx", "gy", "gz"))
    return jax.shard_map(
        shards,
        mesh=mesh,
        in_specs=placed,
        out_specs=(P("gx", "gy", "gz"), P("gx", "gy", "gz")),
        check_vma=False,
    )
```

```python
import functools

import jax
import jax.numpy as jnp
from jax import lax
from jax.experimental import pallas as pl
from jax.experimental.pallas import tpu as pltpu
from jax.sharding import PartitionSpec as P

ITERS = 3
H = ITERS
SEG = 16
PIECES = 4

step_length = 0.5
tv_weight = 0.2
dual_step = 0.28
primal_step = 0.28
MESH = pl.DeviceIdType.MESH


def geometry(dims):
    nx, ny, nz, slots, bx, by, bz = dims
    win = bx + H * min(2, nx - 1)
    tiles = -(-win // (bz // SEG))
    yp = -(-(by + 2 * H) // 8) * 8
    return win, tiles, yp, 16 + (win + tiles) * yp


def own_offset(nx, bx, win, q):
    if nx == 1:
        return 0
    return jnp.where(q == 0, 0, jnp.where(q == nx - 1, win - bx, H))


def roll(value, shift):
    shift = shift % value.shape[1]
    return value if shift == 0 else pltpu.roll(value, shift, 1)


def kernel(
    dims,
    partials,
    code_bits,
    group_map,
    velocity,
    va,
    ga,
    gw,
    scale_out,
    bits,
    gmap,
    part,
    psum,
    vw,
    xr,
    xh,
    ys,
    yr,
    ss,
    zr,
    ds,
    dr,
    za,
    ar,
    in_sem,
    part_sem,
    xs_sem,
    xr_sem,
    xhs_sem,
    xhr_sem,
    vs_sem,
    vr_sem,
    hs_sem,
    hr_sem,
    ars_sem,
    arr_sem,
    chain_sem,
):
    nx, ny, nz, slots, bx, by, bz = dims
    win, tiles, yp, flat = geometry(dims)
    groups = bz // SEG
    ix, iy, iz = lax.axis_index("gx"), lax.axis_index("gy"), lax.axis_index("gz")
    offset = functools.partial(own_offset, nx, bx, win)
    off = offset(ix)
    size = bx // PIECES
    order = [(d, p) for d in list(range(1, nx)) + [0] for p in range(PIECES)]

    def first_row(d, p):
        return lax.rem(ix + d, nx) * bx + p * size

    in_copies = [
        pltpu.make_async_copy(code_bits, bits, in_sem.at[0]),
        pltpu.make_async_copy(group_map, gmap, in_sem.at[1]),
    ]
    v_copy = pltpu.make_async_copy(velocity, vw.at[pl.ds(off, bx)], in_sem.at[2])
    for c in in_copies:
        c.start()
    v_copy.start()
    part_copies = []
    for n, (d, p) in enumerate(order):
        where = pl.ds(first_row(d, p), size)
        part_copies.append(
            pltpu.make_async_copy(partials.at[:, where], part.at[:, where], part_sem.at[n])
        )
    for c in part_copies:
        c.start()

    barrier = pltpu.get_barrier_semaphore()

    def at(x=None, y=None, z=None):
        return (ix if x is None else x, iy if y is None else y, iz if z is None else z)

    def notify(sem, device):
        pl.semaphore_signal(sem, inc=1, device_id=device, device_id_type=MESH)

    for buffer in (yr, zr, dr):
        buffer[...] = jnp.zeros_like(buffer)

    for d in range(1, nx):
        notify(barrier, at(x=lax.rem(ix + d, nx)))
    has = {
        "y-": iy > 0,
        "y+": iy < ny - 1,
        "z-": iz > 0,
        "z+": iz < nz - 1,
    }
    near = {
        "y-": at(y=iy - 1),
        "y+": at(y=iy + 1),
        "z-": at(z=iz - 1),
        "z+": at(z=iz + 1),
    }
    total = jnp.int32(nx - 1)
    for key in has:
        total = total + has[key].astype(jnp.int32)

        @pl.when(has[key])
        def _(key=key):
            notify(barrier, near[key])

    for buffer in (za, va, ga):
        buffer[...] = jnp.zeros_like(buffer)
    pl.semaphore_wait(barrier, total)

    def v_halo(side):
        q = ix + 1 if side == 0 else ix - 1
        src = off + bx - H if side == 0 else off
        dst = offset(q) - H if side == 0 else offset(q) + bx
        return pltpu.make_async_remote_copy(
            src_ref=vw.at[pl.ds(src, H)],
            dst_ref=vw.at[pl.ds(dst, H)],
            send_sem=vs_sem.at[side],
            recv_sem=vr_sem.at[side],
            device_id=at(x=q),
            device_id_type=MESH,
        )

    v_copy.wait()
    if nx > 1:
        @pl.when(ix < nx - 1)
        def _():
            v_halo(0).start()

        @pl.when(ix > 0)
        def _():
            v_halo(1).start()

    for c in in_copies:
        c.wait()
    codes = [gmap[ix * slots + s] for s in range(slots)]

    def reduce_rows(first):
        def one(r, carry):
            row = first + r
            acc = None
            for s in range(slots):
                sign = (2 * bits[codes[s], row] - 1).astype(jnp.float32)
                term = sign * part[s, row]
                acc = term if acc is None else acc + term
            psum[row] = acc
            return carry

        lax.fori_loop(0, size, one, 0, unroll=2)

    def x_copy(d, p):
        return pltpu.make_async_remote_copy(
            src_ref=psum.at[pl.ds(first_row(d, p), size)],
            dst_ref=xr.at[d - 1, pl.ds(p * size, size)],
            send_sem=xs_sem.at[d - 1, p],
            recv_sem=xr_sem.at[d - 1, p],
            device_id=at(x=lax.rem(ix + d, nx)),
            device_id_type=MESH,
        )

    for n, (d, p) in enumerate(order):
        part_copies[n].wait()
        reduce_rows(first_row(d, p))
        if d > 0:
            x_copy(d, p).start()

    def halo_copy(d, side):
        q = lax.rem(ix + d, nx)
        first = q * bx - H if side == 0 else q * bx + bx
        return pltpu.make_async_remote_copy(
            src_ref=psum.at[pl.ds(first, H)],
            dst_ref=xh.at[d - 1, side],
            send_sem=xhs_sem.at[d - 1, side],
            recv_sem=xhr_sem.at[d - 1, side],
            device_id=at(x=q),
            device_id_type=MESH,
        )

    for d in range(1, nx):
        q = lax.rem(ix + d, nx)

        @pl.when(q > 0)
        def _(d=d):
            halo_copy(d, 0).start()

        @pl.when(q < nx - 1)
        def _(d=d):
            halo_copy(d, 1).start()

    def chain(up, down, count, index, sems):
        if count == 1:
            return

        @pl.when(index > 0)
        def _():
            pl.semaphore_wait(chain_sem.at[sems], 1)

        @pl.when(index < count - 1)
        def _():
            notify(chain_sem.at[sems], up)
            pl.semaphore_wait(chain_sem.at[sems + 1], 1)

        @pl.when(index > 0)
        def _():
            notify(chain_sem.at[sems + 1], down)

    chain(near["y+"], near["y-"], ny, iy, 0)
    chain(near["z+"], near["z-"], nz, iz, 2)
    for d in range(1, nx):
        notify(chain_sem.at[4], at(x=lax.rem(ix + d, nx)))

    squares = jnp.zeros((by, bz), jnp.float32)
    for p in range(PIECES):
        for d in range(1, nx):
            x_copy(d, p).wait_recv()
        for r in range(p * size, (p + 1) * size):
            row = psum[ix * bx + r]
            for d in range(1, nx):
                row = row + xr[d - 1, r]
            gw[off + r] = row
            squares = squares + row * row
    count = nx * ny * nz
    me = (ix * ny + iy) * nz + iz
    ar[me] = jnp.sum(squares, axis=0, keepdims=True)
    if nx > 1:
        pl.semaphore_wait(chain_sem.at[4], nx - 1)

    def send_square(d, carry):
        other = lax.rem(me + d, count)
        pltpu.make_async_remote_copy(
            src_ref=ar.at[me],
            dst_ref=ar.at[me],
            send_sem=ars_sem,
            recv_sem=arr_sem,
            device_id=(other // (ny * nz), lax.rem(other // nz, ny), lax.rem(other, nz)),
            device_id_type=MESH,
        ).start()
        return carry

    if count <= 64:
        for d in range(count - 1, 0, -1):
            send_square(d, 0)
    else:
        lax.fori_loop(1, count, send_square, 0)

    for side in range(2):
        if nx == 1:
            break
        present = ix > 0 if side == 0 else ix < nx - 1

        @pl.when(present)
        def _(side=side):
            for d in range(1, nx):
                zone = xh.at[d - 1, side]
                pltpu.make_async_copy(zone, zone, xhr_sem.at[d - 1, side]).wait()
            zone = vw.at[pl.ds(off - H if side == 0 else off + bx, H)]
            pltpu.make_async_copy(zone, zone, vr_sem.at[side]).wait()
            for r in range(H):
                there = ix * bx - H + r if side == 0 else ix * bx + bx + r
                row = psum[there]
                for d in range(1, nx):
                    row = row + xh[d - 1, side, r]
                gw[(off - H if side == 0 else off + bx) + r] = row

    lane = lax.broadcasted_iota(jnp.int32, (1, bz), 1)
    group = lane // SEG
    spot = lax.rem(lane, SEG)

    def pack(read, k):
        acc = None
        for g in range(groups):
            x = tiles * g + k
            if x >= win:
                continue
            moved = roll(read(x), H + SEG * g)
            acc = moved if acc is None else jnp.where(group == g, moved, acc)
        return acc

    fields = (vw, gw)
    for f, field in enumerate(fields):
        for x in range(win):
            tile = field[x]
            ys[0, f, x * H : x * H + H] = tile[by - H : by]
            ys[1, f, x * H : x * H + H] = tile[0:H]
        for k in range(tiles):
            tile = pack(lambda x: field[x], k)
            ss[f, k] = tile
            ds[0, f, k * H : k * H + H] = tile[by - H : by]
            ds[1, f, k * H : k * H + H] = tile[0:H]

    def send(src, dst, n, device):
        return pltpu.make_async_remote_copy(
            src_ref=src,
            dst_ref=dst,
            send_sem=hs_sem.at[n],
            recv_sem=hr_sem.at[n],
            device_id=device,
            device_id_type=MESH,
        )

    both = lambda a, b: jnp.logical_and(has[a], has[b])
    exchange = [
        (send(ys.at[0], yr.at[0], 0, near["y+"]), has["y+"], has["y-"]),
        (send(ys.at[1], yr.at[1], 1, near["y-"]), has["y-"], has["y+"]),
        (send(ss, zr.at[0], 2, near["z+"]), has["z+"], has["z-"]),
        (send(ss, zr.at[1], 3, near["z-"]), has["z-"], has["z+"]),
        (send(ds.at[0], dr.at[0], 4, at(y=iy + 1, z=iz + 1)), both("y+", "z+"), both("y-", "z-")),
        (send(ds.at[0], dr.at[1], 5, at(y=iy + 1, z=iz - 1)), both("y+", "z-"), both("y-", "z+")),
        (send(ds.at[1], dr.at[2], 6, at(y=iy - 1, z=iz + 1)), both("y-", "z+"), both("y+", "z-")),
        (send(ds.at[1], dr.at[3], 7, at(y=iy - 1, z=iz - 1)), both("y-", "z-"), both("y+", "z+")),
    ]
    for copy, sends, _ in exchange:
        pl.when(sends)(copy.start)
    for copy, _, receives in exchange:
        pl.when(receives)(copy.wait_recv)

    front = 8

    def base(x):
        return front + x * yp

    for f, (field, whole) in enumerate(((vw, va), (gw, ga))):
        for x in range(win):
            b = base(x)
            whole[b + H : b + H + by] = field[x]
            whole[b : b + H] = yr[0, f, x * H : x * H + H]
            whole[b + H + by : b + 2 * H + by] = yr[1, f, x * H : x * H + H]
        for k in range(tiles):
            for z in range(2):
                za[z, H : H + by] = zr[z, f, k]
                za[z, 0:H] = dr[z, f, k * H : k * H + H]
                za[z, H + by : 2 * H + by] = dr[2 + z, f, k * H : k * H + H]
            left = za[0, 0:yp]
            mine = pack(lambda x: whole[base(x) : base(x) + yp], k)
            right = roll(za[1, 0:yp], SEG // 2)
            b = base(win + k)
            whole[b : b + yp] = jnp.where(
                spot < H,
                left,
                jnp.where(
                    spot < SEG // 2,
                    mine,
                    jnp.where(spot < SEG // 2 + H, roll(mine, SEG // 2), right),
                ),
            )

    many = ar.at[pl.ds(0, count - 1)]
    pltpu.make_async_copy(many, many, arr_sem).wait()
    square_sum = jnp.sum(jnp.sum(ar[...], axis=0), axis=1, keepdims=True)
    cells = nx * ny * nz * bx * by * bz
    scale = step_length * lax.rsqrt(square_sum / cells + 1.0)

    scale_out[...] = jnp.broadcast_to(scale, scale_out.shape)

    for d in range(1, nx):
        for p in range(PIECES):
            x_copy(d, p).wait_send()
        q = lax.rem(ix + d, nx)
        pl.when(q > 0)(halo_copy(d, 0).wait_send)
        pl.when(q < nx - 1)(halo_copy(d, 1).wait_send)
    if nx > 1:
        pl.when(ix < nx - 1)(v_halo(0).wait_send)
        pl.when(ix > 0)(v_halo(1).wait_send)
    for copy, sends, _ in exchange:
        pl.when(sends)(copy.wait_send)
    pltpu.make_async_copy(many, many, ars_sem).wait()


def proximal(
    dims,
    va,
    ga,
    gw,
    scale_in,
    gradient_out,
    model_out,
    target,
    current,
    extra,
    dx,
    dy,
    dz,
    result,
    out_sem,
):
    nx, ny, nz, slots, bx, by, bz = dims
    win, tiles, yp, flat = geometry(dims)
    ix, iy, iz = lax.axis_index("gx"), lax.axis_index("gy"), lax.axis_index("gz")
    off = own_offset(nx, bx, win, ix)
    g_out = pltpu.make_async_copy(gw.at[pl.ds(off, bx)], gradient_out, out_sem.at[0])
    g_out.start()
    front = 8

    def base(x):
        return front + x * yp

    edge_rows = jnp.zeros((front, bz), jnp.float32)
    dy[0:front] = edge_rows
    target[flat - front : flat] = edge_rows
    extra[flat - front : flat] = edge_rows
    scale = scale_in[...]
    lane = lax.broadcasted_iota(jnp.int32, (1, bz), 1)
    group = lane // SEG
    spot = lax.rem(lane, SEG)
    y_at = iy * by - H + lax.broadcasted_iota(jnp.int32, (yp, 1), 0)
    keep_y = jnp.logical_and(y_at >= 0, y_at < ny * by - 1)
    keep_y = jnp.broadcast_to(keep_y, (yp, bz))
    z_main = iz * bz + lane
    keep_z_main = jnp.broadcast_to(z_main < nz * bz - 1, (yp, bz))
    z_pack = iz * bz + jnp.where(spot < SEG // 2, spot - H, spot - SEG // 2 + bz - H)
    keep_z_pack = jnp.broadcast_to(
        jnp.logical_and(z_pack >= 0, z_pack < nz * bz - 1), (yp, bz)
    )
    start = ix * bx - off
    blocks = win + tiles

    def rows(ref, x, shift=0):
        return ref[base(x) + shift : base(x) + shift + yp]

    for x in range(blocks):
        value = rows(va, x) - scale * rows(ga, x)
        target[base(x) : base(x) + yp] = value

    for it in range(ITERS):
        now = target if it == 0 else extra
        held = target if it == 0 else current
        last = it == ITERS - 1
        for x in range(blocks):
            here = rows(now, x)
            b = base(x)
            ddy = jnp.where(keep_y, rows(now, x, 1) - here, 0.0)
            if x < win:
                g, k = x // tiles, x % tiles
                edge = roll(rows(now, win + k), bz - 1 - (SEG * g + SEG // 2 + H))
                after = jnp.where(lane == bz - 1, edge, roll(here, -1))
                ddz = jnp.where(keep_z_main, after - here, 0.0)
                if x == win - 1:
                    ddx = jnp.zeros_like(here)
                else:
                    ddx = rows(now, x + 1) - here
            else:
                k = x - win
                ddz = jnp.where(keep_z_pack, roll(here, -1) - here, 0.0)
                if k < tiles - 1:
                    after = rows(now, x + 1)
                else:
                    after = roll(rows(now, win), -SEG)
                ddx = jnp.where(tiles * group + k < win - 1, after - here, 0.0)
            px, py, pz = dual_step * ddx, dual_step * ddy, dual_step * ddz
            if it > 0:
                px, py, pz = rows(dx, x) + px, rows(dy, x) + py, rows(dz, x) + pz
            shrink = jnp.minimum(1.0, tv_weight * lax.rsqrt(px * px + py * py + pz * pz))
            dx[b : b + yp] = px * shrink
            dy[b : b + yp] = py * shrink
            dz[b : b + yp] = pz * shrink
        for x in range(win if last else blocks):
            b = base(x)
            qx, qy, qz = rows(dx, x), rows(dy, x), rows(dz, x)
            spread = qy - rows(dy, x, -1)
            if x < win:
                g, k = x // tiles, x % tiles
                edge = roll(rows(dz, win + k), -(SEG * g + H - 1))
                spread = spread + (qz - jnp.where(lane == 0, edge, roll(qz, 1)))
                spread = spread + (qx if x == 0 else qx - rows(dx, x - 1))
            else:
                k = x - win
                spread = spread + (qz - roll(qz, 1))
                before = rows(dx, x - 1) if k > 0 else roll(rows(dx, blocks - 1), SEG)
                spread = spread + (qx - before)
            old = rows(held, x)
            new = (old + primal_step * (spread + rows(target, x))) * (1.0 / (1.0 + primal_step))
            if last:
                result[x] = new[H : H + by]
            else:
                current[b : b + yp] = new
                extra[b : b + yp] = 2.0 * new - old

    m_out = pltpu.make_async_copy(result.at[pl.ds(off, bx)], model_out, out_sem.at[1])
    m_out.start()
    g_out.wait()
    m_out.wait()


def shards(partials, code_bits, group_map, velocity):
    slots = partials.shape[0]
    bx, by, bz = velocity.shape
    nx, ny, nz = (lax.axis_size(a) for a in ("gx", "gy", "gz"))
    dims = (nx, ny, nz, slots, bx, by, bz)
    win, tiles, yp, flat = geometry(dims)
    strip = -(-(win * H + 5) // 8) * 8
    diag = -(-(tiles * H + 5) // 8) * 8
    f32 = functools.partial(pltpu.VMEM, dtype=jnp.float32)
    peers = max(nx - 1, 1)
    dma = pltpu.SemaphoreType.DMA
    anywhere = pl.BlockSpec(memory_space=pl.ANY)
    near = pl.BlockSpec(memory_space=pltpu.VMEM)
    block = jax.ShapeDtypeStruct(velocity.shape, jnp.float32)
    handed = (f32((flat, bz)), f32((flat, bz)), f32((win, by, bz)), f32((1, bz)))
    assembled = pl.pallas_call(
        functools.partial(kernel, dims),
        out_shape=handed,
        in_specs=[pl.BlockSpec(memory_space=pltpu.HBM)] * 4,
        out_specs=(near,) * 4,
        scratch_shapes=[
            pltpu.SMEM(code_bits.shape, jnp.int32),
            pltpu.SMEM(group_map.shape, jnp.int32),
            f32(partials.shape),
            f32((nx * bx, by, bz)),
            f32((win, by, bz)),
            f32((peers, bx, by, bz)),
            f32((peers, 2, H, by, bz)),
            f32((2, 2, strip, bz)),
            f32((2, 2, strip, bz)),
            f32((2, tiles, by, bz)),
            f32((2, 2, tiles, by, bz)),
            f32((2, 2, diag, bz)),
            f32((4, 2, diag, bz)),
            f32((2, yp + 8, bz)),
            f32((nx * ny * nz, 1, bz)),
            dma((3,)),
            dma((nx * PIECES,)),
            dma((peers, PIECES)),
            dma((peers, PIECES)),
            dma((peers, 2)),
            dma((peers, 2)),
            dma((2,)),
            dma((2,)),
            dma((8,)),
            dma((8,)),
            dma,
            dma,
            pltpu.SemaphoreType.REGULAR((5,)),
        ],
        compiler_params=pltpu.CompilerParams(
            collective_id=0, has_side_effects=True
        ),
    )(partials, code_bits, group_map, velocity)
    return pl.pallas_call(
        functools.partial(proximal, dims),
        out_shape=(block, block),
        in_specs=[near] * 4,
        out_specs=(anywhere, anywhere),
        scratch_shapes=[f32((flat, bz))] * 6 + [f32((win, by, bz)), dma((2,))],
        compiler_params=pltpu.CompilerParams(vmem_limit_bytes=32 * 2**20),
    )(*assembled)


def solution(mesh):
    placed = (P("gx", None, "gy", "gz"), P(), P(), P("gx", "gy", "gz"))
    return jax.shard_map(
        shards,
        mesh=mesh,
        in_specs=placed,
        out_specs=(P("gx", "gy", "gz"), P("gx", "gy", "gz")),
        check_vma=False,
    )
```

```python
import functools

import jax
import jax.numpy as jnp
from jax import lax
from jax.experimental import pallas as pl
from jax.experimental.pallas import tpu as pltpu
from jax.sharding import PartitionSpec as P

ITERS = 3
H = ITERS
SEG = 16
PIECES = 4

step_length = 0.5
tv_weight = 0.2
dual_step = 0.28
primal_step = 0.28
MESH = pl.DeviceIdType.MESH


def geometry(dims):
    nx, ny, nz, slots, bx, by, bz = dims
    win = bx + H * min(2, nx - 1)
    tiles = -(-win // (bz // SEG))
    yp = -(-(by + 2 * H) // 8) * 8
    return win, tiles, yp, 16 + (win + tiles) * yp


def own_offset(nx, bx, win, q):
    if nx == 1:
        return 0
    return jnp.where(q == 0, 0, jnp.where(q == nx - 1, win - bx, H))


def roll(value, shift):
    shift = shift % value.shape[1]
    return value if shift == 0 else pltpu.roll(value, shift, 1)


def kernel(
    dims,
    partials,
    code_bits,
    group_map,
    velocity,
    va,
    ga,
    gw,
    scale_out,
    bits,
    gmap,
    part,
    psum,
    vw,
    xr,
    xh,
    ys,
    yr,
    ss,
    zr,
    ds,
    dr,
    za,
    ar,
    in_sem,
    part_sem,
    xs_sem,
    xr_sem,
    xhs_sem,
    xhr_sem,
    vs_sem,
    vr_sem,
    hs_sem,
    hr_sem,
    ars_sem,
    arr_sem,
    chain_sem,
):
    nx, ny, nz, slots, bx, by, bz = dims
    win, tiles, yp, flat = geometry(dims)
    groups = bz // SEG
    ix, iy, iz = lax.axis_index("gx"), lax.axis_index("gy"), lax.axis_index("gz")
    offset = functools.partial(own_offset, nx, bx, win)
    off = offset(ix)
    size = bx // PIECES
    order = [(d, p) for d in list(range(1, nx)) + [0] for p in range(PIECES)]

    def first_row(d, p):
        return lax.rem(ix + d, nx) * bx + p * size

    in_copies = [
        pltpu.make_async_copy(code_bits, bits, in_sem.at[0]),
        pltpu.make_async_copy(group_map, gmap, in_sem.at[1]),
    ]
    v_copy = pltpu.make_async_copy(velocity, vw.at[pl.ds(off, bx)], in_sem.at[2])
    for c in in_copies:
        c.start()
    v_copy.start()
    part_copies = []
    for n, (d, p) in enumerate(order):
        where = pl.ds(first_row(d, p), size)
        part_copies.append(
            pltpu.make_async_copy(partials.at[:, where], part.at[:, where], part_sem.at[n])
        )
    for c in part_copies:
        c.start()

    barrier = pltpu.get_barrier_semaphore()

    def at(x=None, y=None, z=None):
        return (ix if x is None else x, iy if y is None else y, iz if z is None else z)

    def notify(sem, device):
        pl.semaphore_signal(sem, inc=1, device_id=device, device_id_type=MESH)

    for buffer in (yr, zr, dr):
        buffer[...] = jnp.zeros_like(buffer)

    for d in range(1, nx):
        notify(barrier, at(x=lax.rem(ix + d, nx)))
    has = {
        "y-": iy > 0,
        "y+": iy < ny - 1,
        "z-": iz > 0,
        "z+": iz < nz - 1,
    }
    near = {
        "y-": at(y=iy - 1),
        "y+": at(y=iy + 1),
        "z-": at(z=iz - 1),
        "z+": at(z=iz + 1),
    }
    total = jnp.int32(nx - 1)
    for key in has:
        total = total + has[key].astype(jnp.int32)

        @pl.when(has[key])
        def _(key=key):
            notify(barrier, near[key])

    for buffer in (za, va, ga):
        buffer[...] = jnp.zeros_like(buffer)
    pl.semaphore_wait(barrier, total)

    def v_halo(side):
        q = ix + 1 if side == 0 else ix - 1
        src = off + bx - H if side == 0 else off
        dst = offset(q) - H if side == 0 else offset(q) + bx
        return pltpu.make_async_remote_copy(
            src_ref=vw.at[pl.ds(src, H)],
            dst_ref=vw.at[pl.ds(dst, H)],
            send_sem=vs_sem.at[side],
            recv_sem=vr_sem.at[side],
            device_id=at(x=q),
            device_id_type=MESH,
        )

    v_copy.wait()
    if nx > 1:
        @pl.when(ix < nx - 1)
        def _():
            v_halo(0).start()

        @pl.when(ix > 0)
        def _():
            v_halo(1).start()

    for c in in_copies:
        c.wait()
    codes = [gmap[ix * slots + s] for s in range(slots)]

    def reduce_rows(first):
        def one(r, carry):
            row = first + r
            acc = None
            for s in range(slots):
                sign = (2 * bits[codes[s], row] - 1).astype(jnp.float32)
                term = sign * part[s, row]
                acc = term if acc is None else acc + term
            psum[row] = acc
            return carry

        lax.fori_loop(0, size, one, 0, unroll=2)

    def x_copy(d, p):
        return pltpu.make_async_remote_copy(
            src_ref=psum.at[pl.ds(first_row(d, p), size)],
            dst_ref=xr.at[d - 1, pl.ds(p * size, size)],
            send_sem=xs_sem.at[d - 1, p],
            recv_sem=xr_sem.at[d - 1, p],
            device_id=at(x=lax.rem(ix + d, nx)),
            device_id_type=MESH,
        )

    for n, (d, p) in enumerate(order):
        part_copies[n].wait()
        reduce_rows(first_row(d, p))
        if d > 0:
            x_copy(d, p).start()

    def halo_copy(d, side):
        q = lax.rem(ix + d, nx)
        first = q * bx - H if side == 0 else q * bx + bx
        return pltpu.make_async_remote_copy(
            src_ref=psum.at[pl.ds(first, H)],
            dst_ref=xh.at[d - 1, side],
            send_sem=xhs_sem.at[d - 1, side],
            recv_sem=xhr_sem.at[d - 1, side],
            device_id=at(x=q),
            device_id_type=MESH,
        )

    for d in range(1, nx):
        q = lax.rem(ix + d, nx)

        @pl.when(q > 0)
        def _(d=d):
            halo_copy(d, 0).start()

        @pl.when(q < nx - 1)
        def _(d=d):
            halo_copy(d, 1).start()

    def chain(up, down, count, index, sems):
        if count == 1:
            return

        @pl.when(index > 0)
        def _():
            pl.semaphore_wait(chain_sem.at[sems], 1)

        @pl.when(index < count - 1)
        def _():
            notify(chain_sem.at[sems], up)
            pl.semaphore_wait(chain_sem.at[sems + 1], 1)

        @pl.when(index > 0)
        def _():
            notify(chain_sem.at[sems + 1], down)

    chain(near["y+"], near["y-"], ny, iy, 0)
    chain(near["z+"], near["z-"], nz, iz, 2)
    for d in range(1, nx):
        notify(chain_sem.at[4], at(x=lax.rem(ix + d, nx)))

    lane = lax.broadcasted_iota(jnp.int32, (1, bz), 1)
    group = lane // SEG
    spot = lax.rem(lane, SEG)

    def pack(read, k):
        acc = None
        for g in range(groups):
            x = tiles * g + k
            if x >= win:
                continue
            moved = roll(read(x), H + SEG * g)
            acc = moved if acc is None else jnp.where(group == g, moved, acc)
        return acc

    def prepare(f, field):
        for x in range(win):
            tile = field[x]
            ys[0, f, x * H : x * H + H] = tile[by - H : by]
            ys[1, f, x * H : x * H + H] = tile[0:H]
        for k in range(tiles):
            tile = pack(lambda x: field[x], k)
            ss[f, k] = tile
            ds[0, f, k * H : k * H + H] = tile[by - H : by]
            ds[1, f, k * H : k * H + H] = tile[0:H]

    both = lambda a, b: jnp.logical_and(has[a], has[b])

    def exchange(f):
        def send(src, dst, n, device):
            return pltpu.make_async_remote_copy(
                src_ref=src.at[f],
                dst_ref=dst.at[f],
                send_sem=hs_sem.at[f, n],
                recv_sem=hr_sem.at[f, n],
                device_id=device,
                device_id_type=MESH,
            )

        up, down = ds.at[0], ds.at[1]
        pp, pm = both("y+", "z+"), both("y+", "z-")
        mp, mm = both("y-", "z+"), both("y-", "z-")
        return [
            (send(ys.at[0], yr.at[0], 0, near["y+"]), has["y+"], has["y-"]),
            (send(ys.at[1], yr.at[1], 1, near["y-"]), has["y-"], has["y+"]),
            (send(ss, zr.at[0], 2, near["z+"]), has["z+"], has["z-"]),
            (send(ss, zr.at[1], 3, near["z-"]), has["z-"], has["z+"]),
            (send(up, dr.at[0], 4, at(y=iy + 1, z=iz + 1)), pp, mm),
            (send(up, dr.at[1], 5, at(y=iy + 1, z=iz - 1)), pm, mp),
            (send(down, dr.at[2], 6, at(y=iy - 1, z=iz + 1)), mp, pm),
            (send(down, dr.at[3], 7, at(y=iy - 1, z=iz - 1)), mm, pp),
        ]

    def send_all(f):
        for copy, sends, _ in exchange(f):
            pl.when(sends)(copy.start)

    def receive_all(f):
        for copy, _, receives in exchange(f):
            pl.when(receives)(copy.wait_recv)

    front = 8

    def base(x):
        return front + x * yp

    def assemble(f, field, whole):
        for x in range(win):
            b = base(x)
            whole[b + H : b + H + by] = field[x]
            whole[b : b + H] = yr[0, f, x * H : x * H + H]
            whole[b + H + by : b + 2 * H + by] = yr[1, f, x * H : x * H + H]
        for k in range(tiles):
            for z in range(2):
                za[z, H : H + by] = zr[z, f, k]
                za[z, 0:H] = dr[z, f, k * H : k * H + H]
                za[z, H + by : 2 * H + by] = dr[2 + z, f, k * H : k * H + H]
            left = za[0, 0:yp]
            mine = pack(lambda x: whole[base(x) : base(x) + yp], k)
            right = roll(za[1, 0:yp], SEG // 2)
            b = base(win + k)
            whole[b : b + yp] = jnp.where(
                spot < H,
                left,
                jnp.where(
                    spot < SEG // 2,
                    mine,
                    jnp.where(spot < SEG // 2 + H, roll(mine, SEG // 2), right),
                ),
            )

    if nx > 1:
        for side in range(2):
            zone = vw.at[pl.ds(off - H if side == 0 else off + bx, H)]
            arrived = pltpu.make_async_copy(zone, zone, vr_sem.at[side])
            pl.when(ix > 0 if side == 0 else ix < nx - 1)(arrived.wait)
    prepare(0, vw)
    send_all(0)

    squares = jnp.zeros((by, bz), jnp.float32)
    for p in range(PIECES):
        for d in range(1, nx):
            x_copy(d, p).wait_recv()
        for r in range(p * size, (p + 1) * size):
            row = psum[ix * bx + r]
            for d in range(1, nx):
                row = row + xr[d - 1, r]
            gw[off + r] = row
            squares = squares + row * row
    count = nx * ny * nz
    me = (ix * ny + iy) * nz + iz
    ar[me] = jnp.sum(squares, axis=0, keepdims=True)
    if nx > 1:
        pl.semaphore_wait(chain_sem.at[4], nx - 1)

    def send_square(d, carry):
        other = lax.rem(me + d, count)
        pltpu.make_async_remote_copy(
            src_ref=ar.at[me],
            dst_ref=ar.at[me],
            send_sem=ars_sem,
            recv_sem=arr_sem,
            device_id=(other // (ny * nz), lax.rem(other // nz, ny), lax.rem(other, nz)),
            device_id_type=MESH,
        ).start()
        return carry

    if count <= 64:
        for d in range(count - 1, 0, -1):
            send_square(d, 0)
    else:
        lax.fori_loop(1, count, send_square, 0)

    for side in range(2):
        if nx == 1:
            break
        present = ix > 0 if side == 0 else ix < nx - 1

        @pl.when(present)
        def _(side=side):
            for d in range(1, nx):
                zone = xh.at[d - 1, side]
                pltpu.make_async_copy(zone, zone, xhr_sem.at[d - 1, side]).wait()
            for r in range(H):
                there = ix * bx - H + r if side == 0 else ix * bx + bx + r
                row = psum[there]
                for d in range(1, nx):
                    row = row + xh[d - 1, side, r]
                gw[(off - H if side == 0 else off + bx) + r] = row

    prepare(1, gw)
    send_all(1)
    receive_all(0)
    assemble(0, vw, va)
    receive_all(1)
    assemble(1, gw, ga)

    many = ar.at[pl.ds(0, count - 1)]
    pltpu.make_async_copy(many, many, arr_sem).wait()
    square_sum = jnp.sum(jnp.sum(ar[...], axis=0), axis=1, keepdims=True)
    cells = nx * ny * nz * bx * by * bz
    scale = step_length * lax.rsqrt(square_sum / cells + 1.0)

    scale_out[...] = jnp.broadcast_to(scale, scale_out.shape)

    for d in range(1, nx):
        for p in range(PIECES):
            x_copy(d, p).wait_send()
        q = lax.rem(ix + d, nx)
        pl.when(q > 0)(halo_copy(d, 0).wait_send)
        pl.when(q < nx - 1)(halo_copy(d, 1).wait_send)
    if nx > 1:
        pl.when(ix < nx - 1)(v_halo(0).wait_send)
        pl.when(ix > 0)(v_halo(1).wait_send)
    for f in range(2):
        for copy, sends, _ in exchange(f):
            pl.when(sends)(copy.wait_send)
    pltpu.make_async_copy(many, many, ars_sem).wait()


def proximal(
    dims,
    va,
    ga,
    gw,
    scale_in,
    gradient_out,
    model_out,
    target,
    current,
    extra,
    dx,
    dy,
    dz,
    result,
    out_sem,
):
    nx, ny, nz, slots, bx, by, bz = dims
    win, tiles, yp, flat = geometry(dims)
    ix, iy, iz = lax.axis_index("gx"), lax.axis_index("gy"), lax.axis_index("gz")
    off = own_offset(nx, bx, win, ix)
    g_out = pltpu.make_async_copy(gw.at[pl.ds(off, bx)], gradient_out, out_sem.at[0])
    g_out.start()
    front = 8

    def base(x):
        return front + x * yp

    edge_rows = jnp.zeros((front, bz), jnp.float32)
    dy[0:front] = edge_rows
    target[flat - front : flat] = edge_rows
    extra[flat - front : flat] = edge_rows
    scale = scale_in[...]
    lane = lax.broadcasted_iota(jnp.int32, (1, bz), 1)
    group = lane // SEG
    spot = lax.rem(lane, SEG)
    y_at = iy * by - H + lax.broadcasted_iota(jnp.int32, (yp, 1), 0)
    keep_y = jnp.logical_and(y_at >= 0, y_at < ny * by - 1)
    keep_y = jnp.broadcast_to(keep_y, (yp, bz))
    z_main = iz * bz + lane
    keep_z_main = jnp.broadcast_to(z_main < nz * bz - 1, (yp, bz))
    z_pack = iz * bz + jnp.where(spot < SEG // 2, spot - H, spot - SEG // 2 + bz - H)
    keep_z_pack = jnp.broadcast_to(
        jnp.logical_and(z_pack >= 0, z_pack < nz * bz - 1), (yp, bz)
    )
    start = ix * bx - off
    blocks = win + tiles

    def rows(ref, x, shift=0):
        return ref[base(x) + shift : base(x) + shift + yp]

    for x in range(blocks):
        value = rows(va, x) - scale * rows(ga, x)
        target[base(x) : base(x) + yp] = value

    for it in range(ITERS):
        now = target if it == 0 else extra
        held = target if it == 0 else current
        last = it == ITERS - 1
        for x in range(blocks):
            here = rows(now, x)
            b = base(x)
            ddy = jnp.where(keep_y, rows(now, x, 1) - here, 0.0)
            if x < win:
                g, k = x // tiles, x % tiles
                edge = roll(rows(now, win + k), bz - 1 - (SEG * g + SEG // 2 + H))
                after = jnp.where(lane == bz - 1, edge, roll(here, -1))
                ddz = jnp.where(keep_z_main, after - here, 0.0)
                if x == win - 1:
                    ddx = jnp.zeros_like(here)
                else:
                    ddx = rows(now, x + 1) - here
            else:
                k = x - win
                ddz = jnp.where(keep_z_pack, roll(here, -1) - here, 0.0)
                if k < tiles - 1:
                    after = rows(now, x + 1)
                else:
                    after = roll(rows(now, win), -SEG)
                ddx = jnp.where(tiles * group + k < win - 1, after - here, 0.0)
            px, py, pz = dual_step * ddx, dual_step * ddy, dual_step * ddz
            if it > 0:
                px, py, pz = rows(dx, x) + px, rows(dy, x) + py, rows(dz, x) + pz
            shrink = jnp.minimum(1.0, tv_weight * lax.rsqrt(px * px + py * py + pz * pz))
            dx[b : b + yp] = px * shrink
            dy[b : b + yp] = py * shrink
            dz[b : b + yp] = pz * shrink
        for x in range(win if last else blocks):
            b = base(x)
            qx, qy, qz = rows(dx, x), rows(dy, x), rows(dz, x)
            spread = qy - rows(dy, x, -1)
            if x < win:
                g, k = x // tiles, x % tiles
                edge = roll(rows(dz, win + k), -(SEG * g + H - 1))
                spread = spread + (qz - jnp.where(lane == 0, edge, roll(qz, 1)))
                spread = spread + (qx if x == 0 else qx - rows(dx, x - 1))
            else:
                k = x - win
                spread = spread + (qz - roll(qz, 1))
                before = rows(dx, x - 1) if k > 0 else roll(rows(dx, blocks - 1), SEG)
                spread = spread + (qx - before)
            old = rows(held, x)
            new = (old + primal_step * (spread + rows(target, x))) * (1.0 / (1.0 + primal_step))
            if last:
                result[x] = new[H : H + by]
            else:
                current[b : b + yp] = new
                extra[b : b + yp] = 2.0 * new - old

    m_out = pltpu.make_async_copy(result.at[pl.ds(off, bx)], model_out, out_sem.at[1])
    m_out.start()
    g_out.wait()
    m_out.wait()


def shards(partials, code_bits, group_map, velocity):
    slots = partials.shape[0]
    bx, by, bz = velocity.shape
    nx, ny, nz = (lax.axis_size(a) for a in ("gx", "gy", "gz"))
    dims = (nx, ny, nz, slots, bx, by, bz)
    win, tiles, yp, flat = geometry(dims)
    strip = -(-(win * H + 5) // 8) * 8
    diag = -(-(tiles * H + 5) // 8) * 8
    f32 = functools.partial(pltpu.VMEM, dtype=jnp.float32)
    peers = max(nx - 1, 1)
    dma = pltpu.SemaphoreType.DMA
    anywhere = pl.BlockSpec(memory_space=pl.ANY)
    near = pl.BlockSpec(memory_space=pltpu.VMEM)
    block = jax.ShapeDtypeStruct(velocity.shape, jnp.float32)
    handed = (f32((flat, bz)), f32((flat, bz)), f32((win, by, bz)), f32((1, bz)))
    assembled = pl.pallas_call(
        functools.partial(kernel, dims),
        out_shape=handed,
        in_specs=[pl.BlockSpec(memory_space=pltpu.HBM)] * 4,
        out_specs=(near,) * 4,
        scratch_shapes=[
            pltpu.SMEM(code_bits.shape, jnp.int32),
            pltpu.SMEM(group_map.shape, jnp.int32),
            f32(partials.shape),
            f32((nx * bx, by, bz)),
            f32((win, by, bz)),
            f32((peers, bx, by, bz)),
            f32((peers, 2, H, by, bz)),
            f32((2, 2, strip, bz)),
            f32((2, 2, strip, bz)),
            f32((2, tiles, by, bz)),
            f32((2, 2, tiles, by, bz)),
            f32((2, 2, diag, bz)),
            f32((4, 2, diag, bz)),
            f32((2, yp + 8, bz)),
            f32((nx * ny * nz, 1, bz)),
            dma((3,)),
            dma((nx * PIECES,)),
            dma((peers, PIECES)),
            dma((peers, PIECES)),
            dma((peers, 2)),
            dma((peers, 2)),
            dma((2,)),
            dma((2,)),
            dma((2, 8)),
            dma((2, 8)),
            dma,
            dma,
            pltpu.SemaphoreType.REGULAR((5,)),
        ],
        compiler_params=pltpu.CompilerParams(
            collective_id=0, has_side_effects=True
        ),
    )(partials, code_bits, group_map, velocity)
    return pl.pallas_call(
        functools.partial(proximal, dims),
        out_shape=(block, block),
        in_specs=[near] * 4,
        out_specs=(anywhere, anywhere),
        scratch_shapes=[f32((flat, bz))] * 6 + [f32((win, by, bz)), dma((2,))],
        compiler_params=pltpu.CompilerParams(vmem_limit_bytes=32 * 2**20),
    )(*assembled)


def solution(mesh):
    placed = (P("gx", None, "gy", "gz"), P(), P(), P("gx", "gy", "gz"))
    return jax.shard_map(
        shards,
        mesh=mesh,
        in_specs=placed,
        out_specs=(P("gx", "gy", "gz"), P("gx", "gy", "gz")),
        check_vma=False,
    )
```
